32 devices in a mesh: pp: 4 (over z), tp: 4 (over y, core), ep: 2 (over x).
Axes of the slice: x: 2, y: 2, z: 4, core: 2. Of those that a mesh axis runs over, the one named last changes fastest.
Arguments:
- incoming: bfloat16 [4, 1024, 2048], P('pp', ('tp', 'ep')), may hold values from -6 to 6
- expert_ids: int32 [4, 1024, 2], P('pp', ('tp', 'ep')), may hold values from 0 to 7, all different within a row; in each aligned block of 128 rows (0 to 127, 128 to 255, ..., all dimensions but the last counted through in order) at most 64 rows name the same one
- gate_scores: float32 [4, 1024, 2], P('pp', ('tp', 'ep')), may hold values from 0.05 to 1
- gate_proj: bfloat16 [8, 2048, 768], P(('tp', 'ep')), may hold values from -0.125 to 0.125
- up_proj: bfloat16 [8, 2048, 768], P(('tp', 'ep')), may hold values from -0.125 to 0.125
- down_proj: bfloat16 [8, 768, 2048], P(('tp', 'ep')), may hold values from -0.21875 to 0.21875
Outputs:
- combined: bfloat16 [4, 1024, 2048], P('pp', ('tp', 'ep'))
The draws below stay inside these ranges and needn't reach their ends.
Inputs may be any that keep to these rules, and one draw needn't show every extreme that they name: `expert_ids`: each token names 2 different experts. Among the tokens of one device of one section no expert is named more than 64 times, and in every draw some device's tokens name one expert exactly 64 times.
All inputs are finite; a program needn't handle non-finite values.
Results may differ from the reference program's by a relative error of at most 0.0045.
Values may be sent and summed in bfloat16 or wider, within the bound.
A program may use at most 64 MiB of HBM per device.

```python
import math
import jax
import jax.numpy as jnp
import numpy as np
from jax import lax

D = 2048
FF = 768
TOPK = 2
TOK_DEV = 128
EXPERTS = 8
CAP = 64
TOKENS = 1024
N_PP = 4
N_TP = 4
N_EP = 2


def steps_of(own_key, shape, pieces, low, high):
    def one(axis_at, shards_of):
        steps = jax.random.uniform(jax.random.fold_in(jax.random.fold_in(own_key, 6), axis_at), (shards_of,), jnp.float32, low / len(pieces), high / len(pieces))
        return jnp.repeat(jnp.exp(steps), shape[axis_at] // shards_of).reshape((-1,) + (1,) * (len(shape) - axis_at - 1))

    level = one(*pieces[0])
    for cut in pieces[1:]:
        level = level * one(*cut)
    return level


def deal_out(key, own, number, rows, number_of, top, most, slope):
    sequence = jax.random.permutation(key, number_of)
    heavy_load, ordinary = portions_of(number_of, rows * top, most, slope, True), portions_of(number_of, rows * top, most, slope, False)
    places = jnp.arange(number_of)

    def named(sizes, turn):
        used = int((sizes > 0).sum())
        fixed = max(1, used // 4)
        shifted = fixed + (places - fixed + turn * (used - fixed)) % max(1, number_of - fixed)
        return jnp.zeros((number_of,), jnp.int32).at[sequence[jnp.where(places < fixed, places, shifted)]].set(jnp.asarray(sizes, jnp.int32))

    sizes = jnp.where(number % 4 == 0, named(heavy_load, number // 4), named(ordinary, number - number // 4 - 1))
    mixed = jax.random.permutation(jax.random.fold_in(own, 3), number_of)
    source_of, taker = mixed[0:number_of // 2 * 2:2], mixed[1:number_of // 2 * 2:2]
    margin = jnp.minimum(sizes[source_of] - 1, most - sizes[taker]) // 2
    margin = jnp.where((source_of == sequence[0]) | (taker == sequence[0]) | (sizes[taker] == 0), 0, jnp.maximum(margin, 0))
    shifted = jax.random.randint(jax.random.fold_in(own, 4), (number_of // 2,), 0, 1 << 20) % (margin + 1)
    sizes = sizes.at[source_of].add(-shifted).at[taker].add(shifted)
    members = jnp.searchsorted(jnp.cumsum(sizes), jnp.arange(rows * top), side="right").astype(jnp.int32)
    table = members.reshape(top, rows).T
    table = table[jax.random.permutation(jax.random.fold_in(own, 1), rows)]
    turn = jax.random.randint(jax.random.fold_in(own, 2), (rows, 1), 0, top)
    return jnp.take_along_axis(table, (jnp.arange(top)[None, :] + turn) % top, axis=1)


def portions_of(amount, total, most, slope, full):
    portions = [(1 << 20) // math.isqrt(rank ** slope) + 1 for rank in range(1, amount + 1)]
    largest = most if full else min(most, max(-(-total // amount), total * portions[0] // sum(portions)))
    least = 1 if total - largest >= amount - 1 else 0
    holding, rest = [largest] + [least] * (amount - 1), total - largest - least * (amount - 1)
    while rest > 0:
        movable = [i for i in range(1, amount) if holding[i] < largest] or [i for i in range(1, amount) if holding[i] < most]
        pool, budget = sum([portions[i] for i in movable]), rest
        for i in movable:
            addition = min(most - holding[i], max(1, budget * portions[i] // pool), rest)
            holding[i] = holding[i] + addition
            rest = rest - addition
    return np.array(holding)


def noise(key, shape, deviation, most, split=(), kind=jnp.bfloat16):
    loudness = steps_of(key, shape, split, -0.22, 0.18) if split else 1.0
    values = jax.random.normal(key, shape, jnp.float32) * deviation * loudness
    return jnp.minimum(jnp.maximum(values, -most), most).astype(kind)


def setup_inputs(seed: int = 0) -> dict:
    key_list = jax.random.split(jax.random.key(seed), 7)
    incoming = noise(key_list[0], (N_PP, TOKENS, D), 1.0, 6.0, ((0, 4), (1, 8)))
    expert_ids_keys = jax.random.split(jax.random.fold_in(key_list[1], 1), N_PP * TOKENS // TOK_DEV)
    expert_ids_turns = jax.random.permutation(jax.random.fold_in(key_list[1], 3), N_PP * TOKENS // TOK_DEV)
    expert_ids = jax.vmap(lambda own, number: deal_out(jax.random.fold_in(key_list[1], 2), own, number, TOK_DEV, EXPERTS, TOPK, CAP, 2))(expert_ids_keys, expert_ids_turns).reshape((N_PP, TOKENS, TOPK))
    gate_scores = jnp.clip(jnp.exp(math.log(1.0) - 2.9957323 * jax.random.uniform(key_list[2], (N_PP, TOKENS, TOPK), jnp.float32) ** steps_of(key_list[2], (N_PP, TOKENS, TOPK), ((0, 4), (1, 8)), -0.2, 0.2)), 0.05, 1.0)
    gate_proj = noise(key_list[3], (EXPERTS, D, FF), D ** -0.5, 0.125, ((0, 8),))
    up_proj = noise(key_list[4], (EXPERTS, D, FF), D ** -0.5, 0.125, ((0, 8),))
    down_proj = noise(key_list[5], (EXPERTS, FF, D), FF ** -0.5, 0.21875, ((0, 8),))
    return {"incoming": incoming, "expert_ids": expert_ids, "gate_scores": gate_scores, "gate_proj": gate_proj, "up_proj": up_proj, "down_proj": down_proj}


def expert_apply(tokens_in, gate_mat, up_mat, down_mat):
    gate_part = jnp.dot(tokens_in, gate_mat, preferred_element_type=jnp.float32)
    upward = jnp.dot(tokens_in, up_mat, preferred_element_type=jnp.float32)
    hidden = (jax.nn.silu(gate_part) * upward).astype(jnp.bfloat16)
    return jnp.dot(hidden, down_mat, preferred_element_type=jnp.float32).astype(jnp.bfloat16)

def reference(incoming, expert_ids, gate_scores, gate_proj, up_proj, down_proj):
    arrived = jnp.roll(incoming, 1, axis=0).reshape(-1, D)
    values = arrived.astype(jnp.float32)
    normed = (values * lax.rsqrt(lax.optimization_barrier(jnp.mean(values * values, axis=1, keepdims=True)) + 1e-06)).astype(jnp.bfloat16)
    token_total = values.shape[0]
    chosen = expert_ids.reshape(-1).astype(jnp.int32)
    scores = gate_scores.reshape(token_total, TOPK)
    weights = (scores / lax.optimization_barrier(jnp.sum(scores, axis=1, keepdims=True))).reshape(-1)
    assign_total = chosen.shape[0]
    ordering = jnp.argsort(chosen, stable=True).astype(jnp.int32)
    sorted_ids = chosen[ordering]
    counts = jnp.zeros((EXPERTS,), jnp.int32).at[chosen].add(1)
    starts = jnp.cumsum(counts).astype(jnp.int32) - counts
    position = jnp.arange(assign_total, dtype=jnp.int32) - starts[sorted_ids]
    row_bound = N_PP * N_TP * N_EP * CAP
    table_tok = jnp.full((EXPERTS, row_bound), token_total, jnp.int32).at[sorted_ids, position].set(ordering // TOPK)
    table_weight = jnp.zeros((EXPERTS, row_bound), jnp.float32).at[sorted_ids, position].set(weights[ordering])
    with_blank = jnp.concatenate([normed, jnp.zeros((1, D), jnp.bfloat16)], axis=0)

    def per_expert(summed, inputs):
        gate_mat, up_mat, down_mat, tok_list, weight_list = inputs
        answered = expert_apply(with_blank[tok_list], gate_mat, up_mat, down_mat)
        return (summed.at[tok_list].add(weight_list[:, None] * answered.astype(jnp.float32)), None)
    summed, unused = lax.scan(per_expert, jnp.zeros((token_total + 1, D), jnp.float32), (gate_proj, up_proj, down_proj, table_tok, table_weight))
    combined = values + summed[:token_total]
    return combined.astype(jnp.bfloat16).reshape(incoming.shape)
```

```python
import functools

import jax
import jax.numpy as jnp
from jax import lax
from jax.experimental import pallas as pl
from jax.experimental.pallas import tpu as pltpu
from jax.sharding import PartitionSpec as P

MESH = pl.DeviceIdType.MESH
OWN, ACROSS_X, ACROSS_Y, DIAGONAL = range(4)


def shifted(block, axis, distance):
    devices = range(lax.axis_size(axis))
    route = [((i - distance) % len(devices), i) for i in devices]
    return lax.ppermute(block, axis, route)


def expert_apply(tokens_in, gate_mat, up_mat, down_mat):
    gate_part = jnp.dot(tokens_in, gate_mat, preferred_element_type=jnp.float32)
    upward = jnp.dot(tokens_in, up_mat, preferred_element_type=jnp.float32)
    hidden = (jax.nn.silu(gate_part) * upward).astype(jnp.bfloat16)
    return jnp.dot(hidden, down_mat, preferred_element_type=jnp.float32).astype(jnp.bfloat16)


def shards(incoming, expert_ids, gate_scores, gate_proj, up_proj, down_proj):
    arrived = shifted(incoming, "pp", 1)[0]
    tok_count, features = arrived.shape
    top_count = expert_ids.shape[2]
    expert_count = lax.axis_size("tp") * lax.axis_size("ep")
    capacity = min(tok_count, 2 * tok_count * top_count // expert_count)
    values = arrived.astype(jnp.float32)
    normed = (values * lax.rsqrt(jnp.mean(values * values, axis=1, keepdims=True) + 1e-06)).astype(
        jnp.bfloat16
    )
    chosen = expert_ids[0].reshape(-1)
    onehot = (chosen[:, None] == jnp.arange(expert_count, dtype=jnp.int32)[None, :]).astype(
        jnp.int32
    )
    before = jnp.cumsum(onehot, axis=0) - onehot
    slot_of = jnp.sum(before * onehot, axis=1)
    destination = chosen * capacity + slot_of
    owner_row = jnp.arange(chosen.shape[0], dtype=jnp.int32) // top_count
    source_row = (
        jnp.full((expert_count * capacity,), tok_count, jnp.int32).at[destination].set(owner_row)
    )
    occupied = jnp.zeros((expert_count * capacity,), jnp.int32).at[destination].set(1)
    with_blank = jnp.concatenate([normed, jnp.zeros((1, features), jnp.bfloat16)], axis=0)
    outgoing = with_blank[source_row].reshape(expert_count, capacity, features)
    occupied = occupied.reshape(expert_count, capacity)
    gate_mat, up_mat, down_mat = (gate_proj[0], up_proj[0], down_proj[0])
    received_rows = lax.all_to_all(outgoing, ("tp", "ep"), split_axis=0, concat_axis=0, tiled=True)
    flat_rows = received_rows.reshape(-1, features)
    flat_live = lax.all_to_all(
        occupied, ("tp", "ep"), split_axis=0, concat_axis=0, tiled=True
    ).reshape(-1)
    answered = expert_apply(flat_rows, gate_mat, up_mat, down_mat) * flat_live[:, None].astype(
        jnp.bfloat16
    )
    answered = answered.reshape(received_rows.shape)
    returned = lax.all_to_all(answered, ("tp", "ep"), split_axis=0, concat_axis=0, tiled=True)
    picked = returned.reshape(expert_count * capacity, features)[destination].reshape(
        tok_count, top_count, features
    )
    scores = gate_scores[0]
    weights = scores / jnp.sum(scores, axis=1, keepdims=True)
    combined = values + jnp.sum(weights[:, :, None] * picked.astype(jnp.float32), axis=1)
    return combined.astype(jnp.bfloat16)[None]


def exchange_kernel(
    sizes,
    incoming,
    routing,
    gate_hbm,
    up_hbm,
    down_hbm,
    out_ref,
    gate_w,
    up_w,
    down_w,
    tok,
    meta,
    packed,
    hidden,
    kept,
    passed,
    partner,
    to_x,
    to_y,
    to_d,
    from_x,
    from_y,
    via_x,
    via_y,
    total,
    send_sem,
    recv_sem,
    load_sem,
):
    n_pp, n_tp, n_ep, top, cap, chunks, pieces = sizes
    rows, features = tok.shape[2:]
    ff = hidden.shape[1]
    pp, tp, ep = lax.axis_index("pp"), lax.axis_index("tp"), lax.axis_index("ep")
    other_core = tp + 1 - 2 * (tp % 2)
    at_x = {"ep": (ep + 1) % n_ep}
    at_y = {"tp": (tp + 2) % n_tp}
    at_core = {"tp": other_core}
    ahead, behind = {"pp": (pp + 1) % n_pp}, {"pp": (pp + n_pp - 1) % n_pp}

    loads = [
        pltpu.make_async_copy(src.at[0], dst, load_sem.at[i])
        for i, (src, dst) in enumerate(((gate_hbm, gate_w), (up_hbm, up_w), (down_hbm, down_w)))
    ]
    own_meta = pltpu.make_async_copy(routing, meta.at[0], load_sem.at[3])

    barrier = pltpu.get_barrier_semaphore()
    for peer in (at_x, at_y, at_core, ahead, behind):
        pl.semaphore_signal(barrier, inc=1, device_id=peer, device_id_type=MESH)
    own_meta.start()
    pl.semaphore_wait(barrier, 5)

    started = []

    def link(src, dst, peer):
        i = len(started)
        copy = pltpu.make_async_remote_copy(
            src_ref=src,
            dst_ref=dst,
            send_sem=send_sem.at[i],
            recv_sem=recv_sem.at[i],
            device_id=peer,
            device_id_type=MESH,
        )
        started.append(copy)
        copy.start()
        return copy

    size = rows // chunks
    part = [pl.ds(c * size, size) for c in range(chunks)]

    def block(role, side, c):
        return tok.at[role, side, part[c]]

    hop = [link(incoming.at[0, part[c]], block(OWN, 0, c), ahead) for c in range(chunks)]
    for copy in loads:
        copy.start()
    own_meta.wait()
    meta_x = link(meta.at[0], meta.at[2], at_x)
    meta_y = link(meta.at[0], meta.at[4], at_y)
    meta_core = [link(meta.at[0], meta.at[1], at_core)]
    out_x, out_y, out_d, core = {}, {}, {}, {}

    def relay(c):
        out_x[c].wait_recv()
        if c % 2 == 0:
            out_d[c] = link(block(ACROSS_X, 0, c), block(DIAGONAL, 0, c), at_y)
        core[ACROSS_X, c] = link(block(ACROSS_X, 0, c), block(ACROSS_X, 1, c), at_core)
        out_y[c].wait_recv()
        if c % 2 == 1:
            out_d[c] = link(block(ACROSS_Y, 0, c), block(DIAGONAL, 0, c), at_x)
        core[ACROSS_Y, c] = link(block(ACROSS_Y, 0, c), block(ACROSS_Y, 1, c), at_core)

    def relay_diagonal(c):
        out_d[c].wait_recv()
        core[DIAGONAL, c] = link(block(DIAGONAL, 0, c), block(DIAGONAL, 1, c), at_core)

    lag = 2
    for c in range(chunks):
        hop[c].wait_recv()
        out_x[c] = link(block(OWN, 0, c), block(ACROSS_X, 0, c), at_x)
        out_y[c] = link(block(OWN, 0, c), block(ACROSS_Y, 0, c), at_y)
        core[OWN, c] = link(block(OWN, 0, c), block(OWN, 1, c), at_core)
        if c == 0:
            meta_x.wait_recv()
            meta_d = link(meta.at[2], meta.at[6], at_y)
            meta_core.append(link(meta.at[2], meta.at[3], at_core))
            meta_y.wait_recv()
            meta_core.append(link(meta.at[4], meta.at[5], at_core))
        if c == 1:
            meta_d.wait_recv()
            meta_core.append(link(meta.at[6], meta.at[7], at_core))
        if c >= lag:
            relay(c - lag)
    for copy in meta_core:
        copy.wait_recv()

    lane = lax.broadcasted_iota(jnp.int32, (rows, rows), 1)
    earlier = (lax.broadcasted_iota(jnp.int32, (rows, rows), 0) < lane).astype(jnp.bfloat16)
    ids = [meta[:, k, :] for k in range(top)]
    scores = [meta[:, top + k, :] for k in range(top)]
    score_sum = functools.reduce(jnp.add, scores)

    def ranks(expert):
        named = [i == expert for i in ids]
        any_named = functools.reduce(jnp.logical_or, named)
        before = jnp.dot(
            any_named.astype(jnp.float32).astype(jnp.bfloat16),
            earlier,
            preferred_element_type=jnp.float32,
        )
        score = sum(jnp.where(n, s, 0.0) for n, s in zip(named, scores))
        return jnp.where(any_named, before, -1.0), score / score_sum

    mine = (tp * n_ep + ep).astype(jnp.float32)
    theirs = (other_core * n_ep + ep).astype(jnp.float32)
    slot_mine, weight_mine = ranks(mine)
    slot_theirs, _ = ranks(theirs)
    slot_index = lax.broadcasted_iota(jnp.int32, (cap, rows), 0).astype(jnp.float32)

    def slots(rank, i):
        return slot_index == rank[i : i + 1, :]

    def pack(role):
        for side in range(2):
            pick = slots(slot_mine, 2 * role + side)
            chosen = jnp.dot(
                pick.astype(jnp.float32).astype(jnp.bfloat16),
                tok[role, side],
                preferred_element_type=jnp.float32,
            )
            scale = lax.rsqrt(jnp.mean(chosen * chosen, axis=1, keepdims=True) + 1e-06)
            packed[role, pl.ds(side * cap, cap)] = (chosen * scale).astype(jnp.bfloat16)

    def expert(role):
        step = 256 if ff % 256 == 0 else 128
        tokens_in = packed[role]
        for n in range(ff // step):
            cols = pl.ds(n * step, step)
            gate = jnp.dot(tokens_in, gate_w[:, cols], preferred_element_type=jnp.float32)
            upward = jnp.dot(tokens_in, up_w[:, cols], preferred_element_type=jnp.float32)
            hidden[:, cols] = (gate / (1.0 + jnp.exp(-gate)) * upward).astype(jnp.bfloat16)
        weight = [
            jnp.sum(
                jnp.where(slots(slot_mine, 2 * role + side), weight_mine[2 * role + side :][:1], 0.0),
                axis=1,
                keepdims=True,
            )
            for side in range(2)
        ]
        inner = hidden[...]
        for n in range(features // 256):
            cols = pl.ds(n * 256, 256)
            y = jnp.dot(inner, down_w[:, cols], preferred_element_type=jnp.float32)
            y = y.astype(jnp.bfloat16).astype(jnp.float32)
            kept[role, :, cols] = (y[:cap] * weight[0]).astype(jnp.bfloat16)
            passed[role, :, cols] = (y[cap:] * weight[1]).astype(jnp.bfloat16)
        return link(passed.at[role], partner.at[role], at_core)

    def spread(role):
        both = jnp.concatenate(
            [slots(slot_mine, 2 * role), slots(slot_theirs, 2 * role)], axis=0
        ).astype(jnp.float32)
        return both.T.astype(jnp.bfloat16)

    def unpack(role, matrix, lo, hi):
        values = jnp.concatenate([kept[role], partner[role]], axis=0)
        return jnp.dot(matrix[lo:hi], values, preferred_element_type=jnp.float32)

    half = rows // 2
    piece = half // pieces
    cuts = [(p * piece, (p + 1) * piece) for p in range(pieces)]
    for c in range(chunks - lag, chunks):
        relay(c)
    for role in (ACROSS_X, ACROSS_Y):
        for c in range(chunks):
            core[role, c].wait_recv()
    pack(ACROSS_X)
    pack(ACROSS_Y)
    for copy in loads:
        copy.wait()
    swap = {ACROSS_X: expert(ACROSS_X)}
    for c in range(chunks // 2):
        relay_diagonal(c)
    swap[ACROSS_Y] = expert(ACROSS_Y)
    for c in range(chunks // 2, chunks):
        relay_diagonal(c)

    last_x, last_y, last_d = [], [], []

    def post(buffer, landing, lo, hi, value, peer, sends):
        buffer[lo:hi] = value.astype(jnp.bfloat16)
        sends.append(link(buffer.at[pl.ds(lo, hi - lo)], landing, peer))

    swap[ACROSS_X].wait_recv()
    spread_x = spread(ACROSS_X)
    for lo, hi in cuts:
        land = from_x.at[pl.ds(lo, piece)]
        post(to_x, land, lo, hi, unpack(ACROSS_X, spread_x, lo, hi), at_x, last_x)
    swap[ACROSS_Y].wait_recv()
    spread_y = spread(ACROSS_Y)
    for lo, hi in cuts:
        lo, hi = lo + half, hi + half
        land = from_y.at[pl.ds(lo, piece)]
        post(to_y, land, lo, hi, unpack(ACROSS_Y, spread_y, lo, hi), at_y, last_y)
    for c in range(chunks):
        core[DIAGONAL, c].wait_recv()
    pack(DIAGONAL)
    swap[DIAGONAL] = expert(DIAGONAL)
    for c in range(chunks):
        core[OWN, c].wait_recv()
    pack(OWN)
    swap[DIAGONAL].wait_recv()
    spread_d = spread(DIAGONAL)
    over_x, over_y = [], []
    for lo, hi in cuts:
        land = via_x.at[pl.ds(lo, piece)]
        post(to_d, land, lo, hi, unpack(DIAGONAL, spread_d, lo, hi), at_x, over_x)
        land = via_y.at[pl.ds(lo, piece)]
        lo, hi = lo + half, hi + half
        post(to_d, land, lo, hi, unpack(DIAGONAL, spread_d, lo, hi), at_y, over_y)
    swap[OWN] = expert(OWN)
    for p, (lo, hi) in enumerate(cuts):
        over_x[p].wait_recv()
        added = via_x[lo:hi].astype(jnp.float32)
        land = from_y.at[pl.ds(lo, piece)]
        post(to_y, land, lo, hi, unpack(ACROSS_Y, spread_y, lo, hi) + added, at_y, last_y)
        over_y[p].wait_recv()
        added = via_y[lo:hi].astype(jnp.float32)
        lo, hi = lo + half, hi + half
        land = from_x.at[pl.ds(lo, piece)]
        post(to_x, land, lo, hi, unpack(ACROSS_X, spread_x, lo, hi) + added, at_x, last_x)
    swap[OWN].wait_recv()
    total[...] = unpack(OWN, spread(OWN), 0, rows) + tok[OWN, 0].astype(jnp.float32)
    for p, (lo, hi) in enumerate(cuts):
        last_x[p].wait_recv()
        total[lo:hi] += from_x[lo:hi].astype(jnp.float32)
        last_y[p].wait_recv()
        total[lo + half : hi + half] += from_y[lo + half : hi + half].astype(jnp.float32)
    for p, (lo, hi) in enumerate(cuts):
        last_y[pieces + p].wait_recv()
        done = total[lo:hi] + from_y[lo:hi].astype(jnp.float32)
        out_ref[0, lo:hi] = done.astype(jnp.bfloat16)
        last_x[pieces + p].wait_recv()
        lo, hi = lo + half, hi + half
        done = total[lo:hi] + from_x[lo:hi].astype(jnp.float32)
        out_ref[0, lo:hi] = done.astype(jnp.bfloat16)
    for copy in started:
        copy.wait_send()


def fused(incoming, expert_ids, gate_scores, gate_proj, up_proj, down_proj):
    _, rows, features = incoming.shape
    top, ff = expert_ids.shape[2], gate_proj.shape[2]
    n_pp, n_tp, n_ep = (lax.axis_size(a) for a in ("pp", "tp", "ep"))
    cap = min(rows, 2 * rows * top // (n_tp * n_ep))
    chunks, pieces = 8, 2
    routing = jnp.concatenate([expert_ids[0].astype(jnp.float32), gate_scores[0]], axis=1).T
    routing = jnp.pad(routing, ((0, -2 * top % 8), (0, 0)))
    hbm, vmem = pl.BlockSpec(memory_space=pl.ANY), pl.BlockSpec(memory_space=pltpu.VMEM)
    narrow = functools.partial(pltpu.VMEM, dtype=jnp.bfloat16)
    copies = 8 * chunks + 7 + 4 + 6 * pieces
    return pl.pallas_call(
        functools.partial(exchange_kernel, (n_pp, n_tp, n_ep, top, cap, chunks, pieces)),
        out_shape=jax.ShapeDtypeStruct(incoming.shape, incoming.dtype),
        in_specs=[hbm] * 5,
        out_specs=vmem,
        scratch_shapes=[
            narrow((features, ff)),
            narrow((features, ff)),
            narrow((ff, features)),
            narrow((4, 2, rows, features)),
            pltpu.VMEM((8,) + routing.shape, jnp.float32),
            narrow((4, 2 * cap, features)),
            narrow((2 * cap, ff)),
            narrow((4, cap, features)),
            narrow((4, cap, features)),
            narrow((4, cap, features)),
            narrow((rows, features)),
            narrow((rows, features)),
            narrow((rows, features)),
            narrow((rows, features)),
            narrow((rows, features)),
            narrow((rows // 2, features)),
            narrow((rows // 2, features)),
            pltpu.VMEM((rows, features), jnp.float32),
            pltpu.SemaphoreType.DMA((copies,)),
            pltpu.SemaphoreType.DMA((copies,)),
            pltpu.SemaphoreType.DMA((4,)),
        ],
        compiler_params=pltpu.CompilerParams(collective_id=0, has_side_effects=True),
    )(incoming, routing, gate_proj, up_proj, down_proj)


def solution(mesh):
    placed = (
        P("pp", ("tp", "ep"), None),
        P("pp", ("tp", "ep"), None),
        P("pp", ("tp", "ep"), None),
        P(("tp", "ep"), None, None),
        P(("tp", "ep"), None, None),
        P(("tp", "ep"), None, None),
    )
    square = mesh.shape["tp"] == 4 and mesh.shape["ep"] == 2 and mesh.shape["pp"] > 1
    return jax.shard_map(
        fused if square else shards,
        mesh=mesh,
        in_specs=placed,
        out_specs=P("pp", ("tp", "ep"), None),
        check_vma=False,
    )
```

```python
import functools

import jax
import jax.numpy as jnp
from jax import lax
from jax.experimental import pallas as pl
from jax.experimental.pallas import tpu as pltpu
from jax.sharding import PartitionSpec as P

MESH = pl.DeviceIdType.MESH
OWN, ACROSS_X, ACROSS_Y, DIAGONAL = range(4)


def shifted(block, axis, distance):
    devices = range(lax.axis_size(axis))
    route = [((i - distance) % len(devices), i) for i in devices]
    return lax.ppermute(block, axis, route)


def expert_apply(tokens_in, gate_mat, up_mat, down_mat):
    gate_part = jnp.dot(tokens_in, gate_mat, preferred_element_type=jnp.float32)
    upward = jnp.dot(tokens_in, up_mat, preferred_element_type=jnp.float32)
    hidden = (jax.nn.silu(gate_part) * upward).astype(jnp.bfloat16)
    return jnp.dot(hidden, down_mat, preferred_element_type=jnp.float32).astype(jnp.bfloat16)


def shards(incoming, expert_ids, gate_scores, gate_proj, up_proj, down_proj):
    arrived = shifted(incoming, "pp", 1)[0]
    tok_count, features = arrived.shape
    top_count = expert_ids.shape[2]
    expert_count = lax.axis_size("tp") * lax.axis_size("ep")
    capacity = min(tok_count, 2 * tok_count * top_count // expert_count)
    values = arrived.astype(jnp.float32)
    normed = (values * lax.rsqrt(jnp.mean(values * values, axis=1, keepdims=True) + 1e-06)).astype(
        jnp.bfloat16
    )
    chosen = expert_ids[0].reshape(-1)
    onehot = (chosen[:, None] == jnp.arange(expert_count, dtype=jnp.int32)[None, :]).astype(
        jnp.int32
    )
    before = jnp.cumsum(onehot, axis=0) - onehot
    slot_of = jnp.sum(before * onehot, axis=1)
    destination = chosen * capacity + slot_of
    owner_row = jnp.arange(chosen.shape[0], dtype=jnp.int32) // top_count
    source_row = (
        jnp.full((expert_count * capacity,), tok_count, jnp.int32).at[destination].set(owner_row)
    )
    occupied = jnp.zeros((expert_count * capacity,), jnp.int32).at[destination].set(1)
    with_blank = jnp.concatenate([normed, jnp.zeros((1, features), jnp.bfloat16)], axis=0)
    outgoing = with_blank[source_row].reshape(expert_count, capacity, features)
    occupied = occupied.reshape(expert_count, capacity)
    gate_mat, up_mat, down_mat = (gate_proj[0], up_proj[0], down_proj[0])
    received_rows = lax.all_to_all(outgoing, ("tp", "ep"), split_axis=0, concat_axis=0, tiled=True)
    flat_rows = received_rows.reshape(-1, features)
    flat_live = lax.all_to_all(
        occupied, ("tp", "ep"), split_axis=0, concat_axis=0, tiled=True
    ).reshape(-1)
    answered = expert_apply(flat_rows, gate_mat, up_mat, down_mat) * flat_live[:, None].astype(
        jnp.bfloat16
    )
    answered = answered.reshape(received_rows.shape)
    returned = lax.all_to_all(answered, ("tp", "ep"), split_axis=0, concat_axis=0, tiled=True)
    picked = returned.reshape(expert_count * capacity, features)[destination].reshape(
        tok_count, top_count, features
    )
    scores = gate_scores[0]
    weights = scores / jnp.sum(scores, axis=1, keepdims=True)
    combined = values + jnp.sum(weights[:, :, None] * picked.astype(jnp.float32), axis=1)
    return combined.astype(jnp.bfloat16)[None]


def exchange_kernel(
    sizes,
    incoming,
    ids_hbm,
    scores_hbm,
    gate_hbm,
    up_hbm,
    down_hbm,
    out_ref,
    gate_w,
    up_w,
    down_w,
    tok,
    meta_ids,
    meta_scores,
    packed,
    hidden,
    kept,
    passed,
    partner,
    to_x,
    to_y,
    to_d,
    from_x,
    from_y,
    via_x,
    via_y,
    total,
    send_sem,
    recv_sem,
    load_sem,
):
    n_pp, n_tp, n_ep, top, cap, chunks, pieces = sizes
    rows, features = tok.shape[2:]
    ff = hidden.shape[1]
    pp, tp, ep = lax.axis_index("pp"), lax.axis_index("tp"), lax.axis_index("ep")
    other_core = tp + 1 - 2 * (tp % 2)
    at_x = {"ep": (ep + 1) % n_ep}
    at_y = {"tp": (tp + 2) % n_tp}
    at_core = {"tp": other_core}
    ahead, behind = {"pp": (pp + 1) % n_pp}, {"pp": (pp + n_pp - 1) % n_pp}

    splits = 3 * chunks
    loads = []
    for src, dst in ((gate_hbm, gate_w), (up_hbm, up_w), (down_hbm, down_w)):
        depth = dst.shape[0] // chunks
        for c in range(chunks):
            cut = pl.ds(c * depth, depth)
            loads.append(pltpu.make_async_copy(src.at[0, cut], dst.at[cut], load_sem.at[len(loads)]))
    own_meta = [
        pltpu.make_async_copy(ids_hbm, meta_ids.at[0], load_sem.at[splits]),
        pltpu.make_async_copy(scores_hbm, meta_scores.at[0], load_sem.at[splits + 1]),
    ]

    barrier = pltpu.get_barrier_semaphore()
    for peer in (at_x, at_y, at_core, ahead, behind):
        pl.semaphore_signal(barrier, inc=1, device_id=peer, device_id_type=MESH)
    for copy in own_meta:
        copy.start()
    pl.semaphore_wait(barrier, 5)

    started = []

    def link(src, dst, peer):
        i = len(started)
        copy = pltpu.make_async_remote_copy(
            src_ref=src,
            dst_ref=dst,
            send_sem=send_sem.at[i],
            recv_sem=recv_sem.at[i],
            device_id=peer,
            device_id_type=MESH,
        )
        started.append(copy)
        copy.start()
        return copy

    size = rows // chunks
    part = [pl.ds(c * size, size) for c in range(chunks)]

    def block(role, side, c):
        return tok.at[role, side, part[c]]

    hop = [link(incoming.at[0, part[c]], block(OWN, 0, c), ahead) for c in range(chunks)]
    for copy in own_meta:
        copy.wait()

    def meta_link(src, dst, peer):
        return [link(m.at[src], m.at[dst], peer) for m in (meta_ids, meta_scores)]

    meta_x = meta_link(0, 2, at_x)
    meta_y = meta_link(0, 4, at_y)
    meta_core = meta_link(0, 1, at_core)
    out_x, out_y, out_d, core = {}, {}, {}, {}

    def relay(c):
        out_x[c].wait_recv()
        if c % 2 == 0:
            out_d[c] = link(block(ACROSS_X, 0, c), block(DIAGONAL, 0, c), at_y)
        core[ACROSS_X, c] = link(block(ACROSS_X, 0, c), block(ACROSS_X, 1, c), at_core)
        out_y[c].wait_recv()
        if c % 2 == 1:
            out_d[c] = link(block(ACROSS_Y, 0, c), block(DIAGONAL, 0, c), at_x)
        core[ACROSS_Y, c] = link(block(ACROSS_Y, 0, c), block(ACROSS_Y, 1, c), at_core)

    def relay_diagonal(c):
        out_d[c].wait_recv()
        core[DIAGONAL, c] = link(block(DIAGONAL, 0, c), block(DIAGONAL, 1, c), at_core)

    lag = 2
    for c in range(chunks):
        hop[c].wait_recv()
        out_x[c] = link(block(OWN, 0, c), block(ACROSS_X, 0, c), at_x)
        out_y[c] = link(block(OWN, 0, c), block(ACROSS_Y, 0, c), at_y)
        core[OWN, c] = link(block(OWN, 0, c), block(OWN, 1, c), at_core)
        if c == 0:
            for copy in meta_x:
                copy.wait_recv()
            meta_d = meta_link(2, 6, at_y)
            meta_core += meta_link(2, 3, at_core)
            for copy in meta_y:
                copy.wait_recv()
            meta_core += meta_link(4, 5, at_core)
        if c == 1:
            for copy in meta_d:
                copy.wait_recv()
            meta_core += meta_link(6, 7, at_core)
        for copy in loads[c::chunks]:
            copy.start()
        if c >= lag:
            relay(c - lag)
    for copy in meta_core:
        copy.wait_recv()

    lane = lax.broadcasted_iota(jnp.int32, (rows, rows), 1)
    earlier = (lax.broadcasted_iota(jnp.int32, (rows, rows), 0) < lane).astype(jnp.bfloat16)
    ids = [meta_ids[:, k, :] for k in range(top)]
    scores = [meta_scores[:, k, :] for k in range(top)]
    score_sum = functools.reduce(jnp.add, scores)

    def ranks(expert):
        named = [i == expert for i in ids]
        any_named = functools.reduce(jnp.logical_or, named)
        before = jnp.dot(
            any_named.astype(jnp.float32).astype(jnp.bfloat16),
            earlier,
            preferred_element_type=jnp.float32,
        )
        score = sum(jnp.where(n, s, 0.0) for n, s in zip(named, scores))
        return jnp.where(any_named, before, -1.0), score / score_sum

    mine = tp * n_ep + ep
    theirs = other_core * n_ep + ep
    slot_mine, weight_mine = ranks(mine)
    slot_theirs, _ = ranks(theirs)
    slot_index = lax.broadcasted_iota(jnp.int32, (cap, rows), 0).astype(jnp.float32)

    def slots(rank, i):
        return slot_index == rank[i : i + 1, :]

    def pack(role):
        for side in range(2):
            pick = slots(slot_mine, 2 * role + side)
            chosen = jnp.dot(
                pick.astype(jnp.float32).astype(jnp.bfloat16),
                tok[role, side],
                preferred_element_type=jnp.float32,
            )
            scale = lax.rsqrt(jnp.mean(chosen * chosen, axis=1, keepdims=True) + 1e-06)
            packed[role, pl.ds(side * cap, cap)] = (chosen * scale).astype(jnp.bfloat16)

    def expert(role):
        step = 256 if ff % 256 == 0 else 128
        tokens_in = packed[role]
        for n in range(ff // step):
            cols = pl.ds(n * step, step)
            gate = jnp.dot(tokens_in, gate_w[:, cols], preferred_element_type=jnp.float32)
            upward = jnp.dot(tokens_in, up_w[:, cols], preferred_element_type=jnp.float32)
            hidden[:, cols] = (gate / (1.0 + jnp.exp(-gate)) * upward).astype(jnp.bfloat16)
        weight = [
            jnp.sum(
                jnp.where(slots(slot_mine, 2 * role + side), weight_mine[2 * role + side :][:1], 0.0),
                axis=1,
                keepdims=True,
            )
            for side in range(2)
        ]
        inner = hidden[...]
        for n in range(features // 256):
            cols = pl.ds(n * 256, 256)
            y = jnp.dot(inner, down_w[:, cols], preferred_element_type=jnp.float32)
            y = y.astype(jnp.bfloat16).astype(jnp.float32)
            kept[role, :, cols] = (y[:cap] * weight[0]).astype(jnp.bfloat16)
            passed[role, :, cols] = (y[cap:] * weight[1]).astype(jnp.bfloat16)
        return link(passed.at[role], partner.at[role], at_core)

    def spread(role):
        both = jnp.concatenate(
            [slots(slot_mine, 2 * role), slots(slot_theirs, 2 * role)], axis=0
        ).astype(jnp.float32)
        return both.T.astype(jnp.bfloat16)

    def unpack(role, matrix, lo, hi):
        values = jnp.concatenate([kept[role], partner[role]], axis=0)
        return jnp.dot(matrix[lo:hi], values, preferred_element_type=jnp.float32)

    half = rows // 2
    piece = half // pieces
    cuts = [(p * piece, (p + 1) * piece) for p in range(pieces)]
    for c in range(chunks - lag, chunks):
        relay(c)
    for role in (ACROSS_X, ACROSS_Y):
        for c in range(chunks):
            core[role, c].wait_recv()
    pack(ACROSS_X)
    pack(ACROSS_Y)
    for copy in loads:
        copy.wait()
    swap = {ACROSS_X: expert(ACROSS_X)}
    for c in range(chunks // 2):
        relay_diagonal(c)
    swap[ACROSS_Y] = expert(ACROSS_Y)
    for c in range(chunks // 2, chunks):
        relay_diagonal(c)

    last_x, last_y, last_d = [], [], []

    def post(buffer, landing, lo, hi, value, peer, sends):
        buffer[lo:hi] = value.astype(jnp.bfloat16)
        sends.append(link(buffer.at[pl.ds(lo, hi - lo)], landing, peer))

    swap[ACROSS_X].wait_recv()
    spread_x = spread(ACROSS_X)
    for lo, hi in cuts:
        land = from_x.at[pl.ds(lo, piece)]
        post(to_x, land, lo, hi, unpack(ACROSS_X, spread_x, lo, hi), at_x, last_x)
    swap[ACROSS_Y].wait_recv()
    spread_y = spread(ACROSS_Y)
    for lo, hi in cuts:
        lo, hi = lo + half, hi + half
        land = from_y.at[pl.ds(lo, piece)]
        post(to_y, land, lo, hi, unpack(ACROSS_Y, spread_y, lo, hi), at_y, last_y)
    for c in range(chunks):
        core[DIAGONAL, c].wait_recv()
    pack(DIAGONAL)
    swap[DIAGONAL] = expert(DIAGONAL)
    for c in range(chunks):
        core[OWN, c].wait_recv()
    pack(OWN)
    swap[DIAGONAL].wait_recv()
    spread_d = spread(DIAGONAL)
    over_x, over_y = [], []
    for lo, hi in cuts:
        land = via_x.at[pl.ds(lo, piece)]
        post(to_d, land, lo, hi, unpack(DIAGONAL, spread_d, lo, hi), at_x, over_x)
        land = via_y.at[pl.ds(lo, piece)]
        lo, hi = lo + half, hi + half
        post(to_d, land, lo, hi, unpack(DIAGONAL, spread_d, lo, hi), at_y, over_y)
    swap[OWN] = expert(OWN)
    for p, (lo, hi) in enumerate(cuts):
        over_x[p].wait_recv()
        added = via_x[lo:hi].astype(jnp.float32)
        land = from_y.at[pl.ds(lo, piece)]
        post(to_y, land, lo, hi, unpack(ACROSS_Y, spread_y, lo, hi) + added, at_y, last_y)
        over_y[p].wait_recv()
        added = via_y[lo:hi].astype(jnp.float32)
        lo, hi = lo + half, hi + half
        land = from_x.at[pl.ds(lo, piece)]
        post(to_x, land, lo, hi, unpack(ACROSS_X, spread_x, lo, hi) + added, at_x, last_x)
    swap[OWN].wait_recv()
    total[...] = unpack(OWN, spread(OWN), 0, rows) + tok[OWN, 0].astype(jnp.float32)
    for p, (lo, hi) in enumerate(cuts):
        last_x[p].wait_recv()
        total[lo:hi] += from_x[lo:hi].astype(jnp.float32)
        last_y[p].wait_recv()
        total[lo + half : hi + half] += from_y[lo + half : hi + half].astype(jnp.float32)
    for p, (lo, hi) in enumerate(cuts):
        last_y[pieces + p].wait_recv()
        done = total[lo:hi] + from_y[lo:hi].astype(jnp.float32)
        out_ref[0, lo:hi] = done.astype(jnp.bfloat16)
        last_x[pieces + p].wait_recv()
        lo, hi = lo + half, hi + half
        done = total[lo:hi] + from_x[lo:hi].astype(jnp.float32)
        out_ref[0, lo:hi] = done.astype(jnp.bfloat16)
    for copy in started:
        copy.wait_send()


def fused(incoming, expert_ids, gate_scores, gate_proj, up_proj, down_proj):
    _, rows, features = incoming.shape
    top, ff = expert_ids.shape[2], gate_proj.shape[2]
    n_pp, n_tp, n_ep = (lax.axis_size(a) for a in ("pp", "tp", "ep"))
    cap = min(rows, 2 * rows * top // (n_tp * n_ep))
    chunks, pieces = 8, 2
    hbm, vmem = pl.BlockSpec(memory_space=pl.ANY), pl.BlockSpec(memory_space=pltpu.VMEM)
    narrow = functools.partial(pltpu.VMEM, dtype=jnp.bfloat16)
    copies = 8 * chunks + 2 * 7 + 4 + 6 * pieces
    return pl.pallas_call(
        functools.partial(exchange_kernel, (n_pp, n_tp, n_ep, top, cap, chunks, pieces)),
        out_shape=pltpu.VMEM(incoming.shape, incoming.dtype),
        in_specs=[hbm] * 6,
        out_specs=vmem,
        scratch_shapes=[
            narrow((features, ff)),
            narrow((features, ff)),
            narrow((ff, features)),
            narrow((4, 2, rows, features)),
            pltpu.VMEM((8, top, rows), jnp.int32),
            pltpu.VMEM((8, top, rows), jnp.float32),
            narrow((4, 2 * cap, features)),
            narrow((2 * cap, ff)),
            narrow((4, cap, features)),
            narrow((4, cap, features)),
            narrow((4, cap, features)),
            narrow((rows, features)),
            narrow((rows, features)),
            narrow((rows, features)),
            narrow((rows, features)),
            narrow((rows, features)),
            narrow((rows // 2, features)),
            narrow((rows // 2, features)),
            pltpu.VMEM((rows, features), jnp.float32),
            pltpu.SemaphoreType.DMA((copies,)),
            pltpu.SemaphoreType.DMA((copies,)),
            pltpu.SemaphoreType.DMA((3 * chunks + 2,)),
        ],
        compiler_params=pltpu.CompilerParams(collective_id=0, has_side_effects=True),
    )(incoming, expert_ids[0].T, gate_scores[0].T, gate_proj, up_proj, down_proj)


def solution(mesh):
    placed = (
        P("pp", ("tp", "ep"), None),
        P("pp", ("tp", "ep"), None),
        P("pp", ("tp", "ep"), None),
        P(("tp", "ep"), None, None),
        P(("tp", "ep"), None, None),
        P(("tp", "ep"), None, None),
    )
    square = mesh.shape["tp"] == 4 and mesh.shape["ep"] == 2 and mesh.shape["pp"] > 1
    return jax.shard_map(
        fused if square else shards,
        mesh=mesh,
        in_specs=placed,
        out_specs=P("pp", ("tp", "ep"), None),
        check_vma=False,
    )
```

```python
import functools

import jax
import jax.numpy as jnp
from jax import lax
from jax.experimental import pallas as pl
from jax.experimental.pallas import tpu as pltpu
from jax.sharding import PartitionSpec as P

MESH = pl.DeviceIdType.MESH
OWN, ACROSS_X, ACROSS_Y, DIAGONAL = range(4)


def shifted(block, axis, distance):
    devices = range(lax.axis_size(axis))
    route = [((i - distance) % len(devices), i) for i in devices]
    return lax.ppermute(block, axis, route)


def expert_apply(tokens_in, gate_mat, up_mat, down_mat):
    gate_part = jnp.dot(tokens_in, gate_mat, preferred_element_type=jnp.float32)
    upward = jnp.dot(tokens_in, up_mat, preferred_element_type=jnp.float32)
    hidden = (jax.nn.silu(gate_part) * upward).astype(jnp.bfloat16)
    return jnp.dot(hidden, down_mat, preferred_element_type=jnp.float32).astype(jnp.bfloat16)


def shards(incoming, expert_ids, gate_scores, gate_proj, up_proj, down_proj):
    arrived = shifted(incoming, "pp", 1)[0]
    tok_count, features = arrived.shape
    top_count = expert_ids.shape[2]
    expert_count = lax.axis_size("tp") * lax.axis_size("ep")
    capacity = min(tok_count, 2 * tok_count * top_count // expert_count)
    values = arrived.astype(jnp.float32)
    normed = (values * lax.rsqrt(jnp.mean(values * values, axis=1, keepdims=True) + 1e-06)).astype(
        jnp.bfloat16
    )
    chosen = expert_ids[0].reshape(-1)
    onehot = (chosen[:, None] == jnp.arange(expert_count, dtype=jnp.int32)[None, :]).astype(
        jnp.int32
    )
    before = jnp.cumsum(onehot, axis=0) - onehot
    slot_of = jnp.sum(before * onehot, axis=1)
    destination = chosen * capacity + slot_of
    owner_row = jnp.arange(chosen.shape[0], dtype=jnp.int32) // top_count
    source_row = (
        jnp.full((expert_count * capacity,), tok_count, jnp.int32).at[destination].set(owner_row)
    )
    occupied = jnp.zeros((expert_count * capacity,), jnp.int32).at[destination].set(1)
    with_blank = jnp.concatenate([normed, jnp.zeros((1, features), jnp.bfloat16)], axis=0)
    outgoing = with_blank[source_row].reshape(expert_count, capacity, features)
    occupied = occupied.reshape(expert_count, capacity)
    gate_mat, up_mat, down_mat = (gate_proj[0], up_proj[0], down_proj[0])
    received_rows = lax.all_to_all(outgoing, ("tp", "ep"), split_axis=0, concat_axis=0, tiled=True)
    flat_rows = received_rows.reshape(-1, features)
    flat_live = lax.all_to_all(
        occupied, ("tp", "ep"), split_axis=0, concat_axis=0, tiled=True
    ).reshape(-1)
    answered = expert_apply(flat_rows, gate_mat, up_mat, down_mat) * flat_live[:, None].astype(
        jnp.bfloat16
    )
    answered = answered.reshape(received_rows.shape)
    returned = lax.all_to_all(answered, ("tp", "ep"), split_axis=0, concat_axis=0, tiled=True)
    picked = returned.reshape(expert_count * capacity, features)[destination].reshape(
        tok_count, top_count, features
    )
    scores = gate_scores[0]
    weights = scores / jnp.sum(scores, axis=1, keepdims=True)
    combined = values + jnp.sum(weights[:, :, None] * picked.astype(jnp.float32), axis=1)
    return combined.astype(jnp.bfloat16)[None]


def exchange_kernel(
    sizes,
    incoming,
    ids_hbm,
    scores_hbm,
    gate_hbm,
    up_hbm,
    down_hbm,
    out_ref,
    gate_w,
    up_w,
    down_w,
    tok,
    meta_ids,
    meta_scores,
    packed,
    hidden,
    kept,
    passed,
    partner,
    to_x,
    to_y,
    to_d,
    from_x,
    from_y,
    via_x,
    via_y,
    total,
    send_sem,
    recv_sem,
    load_sem,
):
    n_pp, n_tp, n_ep, top, cap, chunks, pieces = sizes
    rows, features = tok.shape[2:]
    ff = hidden.shape[1]
    pp, tp, ep = lax.axis_index("pp"), lax.axis_index("tp"), lax.axis_index("ep")
    other_core = tp + 1 - 2 * (tp % 2)
    at_x = {"ep": (ep + 1) % n_ep}
    at_y = {"tp": (tp + 2) % n_tp}
    at_core = {"tp": other_core}
    ahead, behind = {"pp": (pp + 1) % n_pp}, {"pp": (pp + n_pp - 1) % n_pp}

    splits = 3 * chunks
    loads = []
    for src, dst in ((gate_hbm, gate_w), (up_hbm, up_w), (down_hbm, down_w)):
        depth = dst.shape[0] // chunks
        for c in range(chunks):
            cut = pl.ds(c * depth, depth)
            loads.append(pltpu.make_async_copy(src.at[0, cut], dst.at[cut], load_sem.at[len(loads)]))
    own_meta = [
        pltpu.make_async_copy(ids_hbm, meta_ids.at[0], load_sem.at[splits]),
        pltpu.make_async_copy(scores_hbm, meta_scores.at[0], load_sem.at[splits + 1]),
    ]

    barrier = pltpu.get_barrier_semaphore()
    for peer in (at_x, at_y, at_core, ahead, behind):
        pl.semaphore_signal(barrier, inc=1, device_id=peer, device_id_type=MESH)
    for copy in own_meta:
        copy.start()
    pl.semaphore_wait(barrier, 5)

    started = []

    def link(src, dst, peer):
        i = len(started)
        copy = pltpu.make_async_remote_copy(
            src_ref=src,
            dst_ref=dst,
            send_sem=send_sem.at[i],
            recv_sem=recv_sem.at[i],
            device_id=peer,
            device_id_type=MESH,
        )
        started.append(copy)
        copy.start()
        return copy

    size = rows // chunks
    part = [pl.ds(c * size, size) for c in range(chunks)]

    def block(role, side, c):
        return tok.at[role, side, part[c]]

    hop = [link(incoming.at[0, part[c]], block(OWN, 0, c), ahead) for c in range(chunks)]
    for copy in own_meta:
        copy.wait()

    def meta_link(src, dst, peer):
        return [link(m.at[src], m.at[dst], peer) for m in (meta_ids, meta_scores)]

    meta_x = meta_link(0, 2, at_x)
    meta_y = meta_link(0, 4, at_y)
    meta_core = meta_link(0, 1, at_core)
    out_x, out_y, out_d, core = {}, {}, {}, {}

    def relay(c):
        out_x[c].wait_recv()
        if c % 2 == 0:
            out_d[c] = link(block(ACROSS_X, 0, c), block(DIAGONAL, 0, c), at_y)
        core[ACROSS_X, c] = link(block(ACROSS_X, 0, c), block(ACROSS_X, 1, c), at_core)
        out_y[c].wait_recv()
        if c % 2 == 1:
            out_d[c] = link(block(ACROSS_Y, 0, c), block(DIAGONAL, 0, c), at_x)
        core[ACROSS_Y, c] = link(block(ACROSS_Y, 0, c), block(ACROSS_Y, 1, c), at_core)

    def relay_diagonal(c):
        out_d[c].wait_recv()
        core[DIAGONAL, c] = link(block(DIAGONAL, 0, c), block(DIAGONAL, 1, c), at_core)

    lag = chunks
    for c in range(chunks):
        hop[c].wait_recv()
        out_x[c] = link(block(OWN, 0, c), block(ACROSS_X, 0, c), at_x)
        out_y[c] = link(block(OWN, 0, c), block(ACROSS_Y, 0, c), at_y)
        core[OWN, c] = link(block(OWN, 0, c), block(OWN, 1, c), at_core)
        if c == 0:
            for copy in meta_x:
                copy.wait_recv()
            meta_d = meta_link(2, 6, at_y)
            meta_core += meta_link(2, 3, at_core)
            for copy in meta_y:
                copy.wait_recv()
            meta_core += meta_link(4, 5, at_core)
        if c == chunks // 2:
            for copy in meta_d:
                copy.wait_recv()
            meta_core += meta_link(6, 7, at_core)
        for copy in loads[c::chunks]:
            copy.start()
        if c >= lag:
            relay(c - lag)
    for copy in meta_core:
        copy.wait_recv()

    lane = lax.broadcasted_iota(jnp.int32, (rows, rows), 1)
    earlier = (lax.broadcasted_iota(jnp.int32, (rows, rows), 0) < lane).astype(jnp.bfloat16)
    ids = [meta_ids[:, k, :] for k in range(top)]
    scores = [meta_scores[:, k, :] for k in range(top)]
    score_sum = functools.reduce(jnp.add, scores)

    def ranks(expert):
        named = [i == expert for i in ids]
        any_named = functools.reduce(jnp.logical_or, named)
        before = jnp.dot(
            any_named.astype(jnp.float32).astype(jnp.bfloat16),
            earlier,
            preferred_element_type=jnp.float32,
        )
        score = sum(jnp.where(n, s, 0.0) for n, s in zip(named, scores))
        return jnp.where(any_named, before, -1.0), score / score_sum

    mine = tp * n_ep + ep
    theirs = other_core * n_ep + ep
    slot_mine, weight_mine = ranks(mine)
    slot_theirs, _ = ranks(theirs)
    slot_index = lax.broadcasted_iota(jnp.int32, (cap, rows), 0).astype(jnp.float32)

    def slots(rank, i):
        return slot_index == rank[i : i + 1, :]

    def pack(role):
        for side in range(2):
            pick = slots(slot_mine, 2 * role + side)
            chosen = jnp.dot(
                pick.astype(jnp.float32).astype(jnp.bfloat16),
                tok[role, side],
                preferred_element_type=jnp.float32,
            )
            scale = lax.rsqrt(jnp.mean(chosen * chosen, axis=1, keepdims=True) + 1e-06)
            packed[role, pl.ds(side * cap, cap)] = (chosen * scale).astype(jnp.bfloat16)

    def expert(role):
        step = 256 if ff % 256 == 0 else 128
        tokens_in = packed[role]
        for n in range(ff // step):
            cols = pl.ds(n * step, step)
            gate = jnp.dot(tokens_in, gate_w[:, cols], preferred_element_type=jnp.float32)
            upward = jnp.dot(tokens_in, up_w[:, cols], preferred_element_type=jnp.float32)
            hidden[:, cols] = (gate / (1.0 + jnp.exp(-gate)) * upward).astype(jnp.bfloat16)
        weight = [
            jnp.sum(
                jnp.where(slots(slot_mine, 2 * role + side), weight_mine[2 * role + side :][:1], 0.0),
                axis=1,
                keepdims=True,
            )
            for side in range(2)
        ]
        inner = hidden[...]
        for n in range(features // 256):
            cols = pl.ds(n * 256, 256)
            y = jnp.dot(inner, down_w[:, cols], preferred_element_type=jnp.float32)
            y = y.astype(jnp.bfloat16).astype(jnp.float32)
            kept[role, :, cols] = (y[:cap] * weight[0]).astype(jnp.bfloat16)
            passed[role, :, cols] = (y[cap:] * weight[1]).astype(jnp.bfloat16)
        return link(passed.at[role], partner.at[role], at_core)

    def spread(role):
        both = jnp.concatenate(
            [slots(slot_mine, 2 * role), slots(slot_theirs, 2 * role)], axis=0
        ).astype(jnp.float32)
        return both.T.astype(jnp.bfloat16)

    def unpack(role, matrix, lo, hi):
        values = jnp.concatenate([kept[role], partner[role]], axis=0)
        return jnp.dot(matrix[lo:hi], values, preferred_element_type=jnp.float32)

    half = rows // 2
    piece = half // pieces
    cuts = [(p * piece, (p + 1) * piece) for p in range(pieces)]
    for c in range(chunks - lag, chunks):
        relay(c)
    for role in (ACROSS_X, ACROSS_Y):
        for c in range(chunks):
            core[role, c].wait_recv()
    pack(ACROSS_X)
    pack(ACROSS_Y)
    for copy in loads:
        copy.wait()
    swap = {ACROSS_X: expert(ACROSS_X)}
    swap[ACROSS_Y] = expert(ACROSS_Y)
    for c in range(chunks):
        relay_diagonal(c)

    last_x, last_y, last_d = [], [], []

    def post(buffer, landing, lo, hi, value, peer, sends):
        buffer[lo:hi] = value.astype(jnp.bfloat16)
        sends.append(link(buffer.at[pl.ds(lo, hi - lo)], landing, peer))

    swap[ACROSS_X].wait_recv()
    spread_x = spread(ACROSS_X)
    for lo, hi in cuts:
        land = from_x.at[pl.ds(lo, piece)]
        post(to_x, land, lo, hi, unpack(ACROSS_X, spread_x, lo, hi), at_x, last_x)
    swap[ACROSS_Y].wait_recv()
    spread_y = spread(ACROSS_Y)
    for lo, hi in cuts:
        lo, hi = lo + half, hi + half
        land = from_y.at[pl.ds(lo, piece)]
        post(to_y, land, lo, hi, unpack(ACROSS_Y, spread_y, lo, hi), at_y, last_y)
    for c in range(chunks):
        core[DIAGONAL, c].wait_recv()
    pack(DIAGONAL)
    swap[DIAGONAL] = expert(DIAGONAL)
    for c in range(chunks):
        core[OWN, c].wait_recv()
    pack(OWN)
    swap[DIAGONAL].wait_recv()
    spread_d = spread(DIAGONAL)
    over_x, over_y = [], []
    for lo, hi in cuts:
        land = via_x.at[pl.ds(lo, piece)]
        post(to_d, land, lo, hi, unpack(DIAGONAL, spread_d, lo, hi), at_x, over_x)
        land = via_y.at[pl.ds(lo, piece)]
        lo, hi = lo + half, hi + half
        post(to_d, land, lo, hi, unpack(DIAGONAL, spread_d, lo, hi), at_y, over_y)
    swap[OWN] = expert(OWN)
    for p, (lo, hi) in enumerate(cuts):
        over_x[p].wait_recv()
        added = via_x[lo:hi].astype(jnp.float32)
        land = from_y.at[pl.ds(lo, piece)]
        post(to_y, land, lo, hi, unpack(ACROSS_Y, spread_y, lo, hi) + added, at_y, last_y)
        over_y[p].wait_recv()
        added = via_y[lo:hi].astype(jnp.float32)
        lo, hi = lo + half, hi + half
        land = from_x.at[pl.ds(lo, piece)]
        post(to_x, land, lo, hi, unpack(ACROSS_X, spread_x, lo, hi) + added, at_x, last_x)
    swap[OWN].wait_recv()
    total[...] = unpack(OWN, spread(OWN), 0, rows) + tok[OWN, 0].astype(jnp.float32)
    for p, (lo, hi) in enumerate(cuts):
        last_x[p].wait_recv()
        total[lo:hi] += from_x[lo:hi].astype(jnp.float32)
        last_y[p].wait_recv()
        total[lo + half : hi + half] += from_y[lo + half : hi + half].astype(jnp.float32)
    for p, (lo, hi) in enumerate(cuts):
        last_y[pieces + p].wait_recv()
        done = total[lo:hi] + from_y[lo:hi].astype(jnp.float32)
        out_ref[0, lo:hi] = done.astype(jnp.bfloat16)
        last_x[pieces + p].wait_recv()
        lo, hi = lo + half, hi + half
        done = total[lo:hi] + from_x[lo:hi].astype(jnp.float32)
        out_ref[0, lo:hi] = done.astype(jnp.bfloat16)
    for copy in started:
        copy.wait_send()


def fused(incoming, expert_ids, gate_scores, gate_proj, up_proj, down_proj):
    _, rows, features = incoming.shape
    top, ff = expert_ids.shape[2], gate_proj.shape[2]
    n_pp, n_tp, n_ep = (lax.axis_size(a) for a in ("pp", "tp", "ep"))
    cap = min(rows, 2 * rows * top // (n_tp * n_ep))
    chunks, pieces = 8, 2
    hbm, vmem = pl.BlockSpec(memory_space=pl.ANY), pl.BlockSpec(memory_space=pltpu.VMEM)
    narrow = functools.partial(pltpu.VMEM, dtype=jnp.bfloat16)
    copies = 8 * chunks + 2 * 7 + 4 + 6 * pieces
    return pl.pallas_call(
        functools.partial(exchange_kernel, (n_pp, n_tp, n_ep, top, cap, chunks, pieces)),
        out_shape=pltpu.VMEM(incoming.shape, incoming.dtype),
        in_specs=[hbm] * 6,
        out_specs=vmem,
        scratch_shapes=[
            narrow((features, ff)),
            narrow((features, ff)),
            narrow((ff, features)),
            narrow((4, 2, rows, features)),
            pltpu.VMEM((8, top, rows), jnp.int32),
            pltpu.VMEM((8, top, rows), jnp.float32),
            narrow((4, 2 * cap, features)),
            narrow((2 * cap, ff)),
            narrow((4, cap, features)),
            narrow((4, cap, features)),
            narrow((4, cap, features)),
            narrow((rows, features)),
            narrow((rows, features)),
            narrow((rows, features)),
            narrow((rows, features)),
            narrow((rows, features)),
            narrow((rows // 2, features)),
            narrow((rows // 2, features)),
            pltpu.VMEM((rows, features), jnp.float32),
            pltpu.SemaphoreType.DMA((copies,)),
            pltpu.SemaphoreType.DMA((copies,)),
            pltpu.SemaphoreType.DMA((3 * chunks + 2,)),
        ],
        compiler_params=pltpu.CompilerParams(collective_id=0, has_side_effects=True),
    )(incoming, expert_ids[0].T, gate_scores[0].T, gate_proj, up_proj, down_proj)


def solution(mesh):
    placed = (
        P("pp", ("tp", "ep"), None),
        P("pp", ("tp", "ep"), None),
        P("pp", ("tp", "ep"), None),
        P(("tp", "ep"), None, None),
        P(("tp", "ep"), None, None),
        P(("tp", "ep"), None, None),
    )
    square = mesh.shape["tp"] == 4 and mesh.shape["ep"] == 2 and mesh.shape["pp"] > 1
    return jax.shard_map(
        fused if square else shards,
        mesh=mesh,
        in_specs=placed,
        out_specs=P("pp", ("tp", "ep"), None),
        check_vma=False,
    )
```
